1024 devices in a mesh: gx: 8 (over z), gy: 16 (over x, core), gz: 8 (over y).
Axes of the slice: x: 8, y: 8, z: 8, core: 2. Of those that a mesh axis runs over, the one named last changes fastest.
Arguments:
- right_side: float32 [32, 128, 1024], P('gx', 'gy', 'gz'), may hold values from -8 to 8
- diagonal: float32 [32, 128, 1024], P('gx', 'gy', 'gz'), may hold values from 0.2 to 2
- sign_bits: int32 [32, 128, 1024], P('gx', 'gy', 'gz'), may hold values from 0 to 1
- freq_x: int32 [2048], replicated, may hold values from 0 to 31
- freq_y: int32 [2048], replicated, may hold values from 0 to 127
- freq_z: int32 [2048], replicated, may hold values from 0 to 1023
Outputs:
- solution_field: float32 [32, 128, 1024], P('gx', 'gy', 'gz')
- residual: float32 [32, 128, 1024], P('gx', 'gy', 'gz')
The draws below stay inside these ranges and needn't reach their ends.
All inputs are finite; a program needn't handle non-finite values.
Results may differ from the reference program's by a relative error of at most 0.0009.
Values sent between devices are 32-bit elements; how exact they have to be, the bound alone decides.
No kernel may reach another device: no remote copies, remote signals or barrier semaphores. Data moves between devices by JAX's collectives and lax.ppermute only.
A program may use at most 32 MiB of HBM per device.

```python
import math
import jax
import jax.numpy as jnp
from jax import lax

BASIS = 8
ITERS = 2
SKETCH = 2048
NX = 32
NY = 128
NZ = 1024


def place_ends(entries, rng, least, largest):
    shape = entries.shape
    index_at = [jax.random.randint(jax.random.fold_in(rng, axis), (), 0, shape[axis]) for axis in range(len(shape))]
    entries = entries.at[tuple(index_at)].set(least)
    longest = shape.index(max(shape))
    index_at[longest] = (index_at[longest] + 1) % shape[longest]
    return entries.at[tuple(index_at)].set(largest)


def block_scale(own_key, shape, shards, least, largest):
    gain, own = 1.0, jax.random.fold_in(own_key, 6)
    for dim, shards_of in shards:
        heights = jnp.exp(jax.random.uniform(jax.random.fold_in(own, dim), (shards_of,), jnp.float32, least / len(shards), largest / len(shards)))
        gain = gain * jnp.repeat(heights, shape[dim] // shards_of).reshape([-1 if axis == dim else 1 for axis in range(len(shape))])
    return gain


def centred(own_key, extent, scale, reach, cuts=(), held_as=jnp.bfloat16):
    drawn = scale * jax.random.normal(own_key, extent, jnp.float32)
    if cuts:
        drawn = drawn * block_scale(own_key, extent, cuts, -0.22, 0.18)
    return jnp.clip(drawn, -reach, reach).astype(held_as)


def setup_inputs(seed: int = 0) -> dict:
    seeds = jax.random.split(jax.random.key(seed), 7)
    return {
        "right_side": centred(seeds[0], (NX, NY, NZ), 1.0, 8.0, ((0, 8), (1, 16), (2, 8)), jnp.float32),
        "diagonal": jnp.clip(jnp.exp(math.log(2.0) - 2.3025851 * jax.random.uniform(seeds[1], (NX, NY, NZ), jnp.float32) ** block_scale(seeds[1], (NX, NY, NZ), ((0, 8), (1, 16), (2, 8)), -0.2, 0.2)), 0.2, 2.0),
        "sign_bits": place_ends(jax.random.randint(seeds[2], (NX, NY, NZ), 0, 2), jax.random.fold_in(seeds[2], 1), 0, 1).astype(jnp.int32),
        "freq_x": place_ends(jax.random.randint(seeds[3], (SKETCH,), 0, NX), jax.random.fold_in(seeds[3], 1), 0, NX - 1).astype(jnp.int32),
        "freq_y": place_ends(jax.random.randint(seeds[4], (SKETCH,), 0, NY), jax.random.fold_in(seeds[4], 1), 0, NY - 1).astype(jnp.int32),
        "freq_z": place_ends(jax.random.randint(seeds[5], (SKETCH,), 0, NZ), jax.random.fold_in(seeds[5], 1), 0, NZ - 1).astype(jnp.int32),
    }


center_value = 7.0
half_range = 7.0
tiny_value = 1e-06
highest = lax.Precision.HIGHEST

def stencil(padded, diagonal):
    beside = padded[2:, 1:-1, 1:-1] + padded[:-2, 1:-1, 1:-1]
    beside = beside + padded[1:-1, 2:, 1:-1] + padded[1:-1, :-2, 1:-1]
    beside = beside + padded[1:-1, 1:-1, 2:] + padded[1:-1, 1:-1, :-2]
    return (6.0 + diagonal) * padded[1:-1, 1:-1, 1:-1] - beside

def cosine_table(freqs, count, length):
    indices = jnp.arange(count, dtype=jnp.int32)
    phases = (2 * indices[:, None] + 1) * freqs[None, :].astype(jnp.int32) % (4 * length)
    return (jnp.sqrt(2.0 / length) * jnp.cos(jnp.pi * phases / (2.0 * length))).astype(jnp.float32)

def least_squares(matrix):
    count = matrix.shape[0] - 1
    target = matrix[count]
    orthonormal = []
    upper = {}
    for column_at in range(count):
        column = matrix[column_at]
        for repeat in range(2):
            for earlier in range(column_at):
                amount = jnp.dot(orthonormal[earlier], column, precision=highest)
                column = column - amount * orthonormal[earlier]
                upper[earlier, column_at] = upper.get((earlier, column_at), 0.0) + amount
        length = jnp.sqrt(jnp.dot(column, column, precision=highest) + tiny_value)
        orthonormal.append(column / length)
        upper[column_at, column_at] = length
    projected = [jnp.dot(basis_row, target, precision=highest) for basis_row in orthonormal]
    solved = [None] * count
    for row_at in range(count - 1, -1, -1):
        value = projected[row_at]
        for later in range(row_at + 1, count):
            value = value - upper[row_at, later] * solved[later]
        solved[row_at] = value / upper[row_at, row_at]
    return jnp.stack(solved)

def chebyshev(residual, diagonal):
    vectors = [residual]
    images = []
    for position in range(BASIS):
        image = stencil(jnp.pad(vectors[position], 1), diagonal)
        images.append(image)
        if position + 1 < BASIS:
            turned = (image - center_value * vectors[position]) / half_range
            vectors.append(turned if position == 0 else 2.0 * turned - vectors[position - 1])
    return (vectors, images)

def sketch(columns, signs, table_x, table_y, table_z):
    flipped = jnp.stack(columns, axis=2) * signs[:, :, None, :]

    def per_slab(carry, inputs):
        slab_rows, row_x = inputs
        inner_sums = jnp.einsum('yjz,zs->yjs', slab_rows, table_z, precision=highest)
        weights = row_x[None, :] * table_y
        return (carry + jnp.einsum('yjs,ys->js', inner_sums, weights, precision=highest), None)
    start = jnp.zeros((len(columns), table_z.shape[1]), jnp.float32)
    summed, _ = lax.scan(per_slab, start, (flipped, table_x))
    return summed

def reference(right_side, diagonal, sign_bits, freq_x, freq_y, freq_z):
    size_x, size_y, size_z = right_side.shape
    table_x = cosine_table(freq_x, size_x, size_x)
    table_y = cosine_table(freq_y, size_y, size_y)
    table_z = cosine_table(freq_z, size_z, size_z)
    signs = 1.0 - 2.0 * sign_bits.astype(jnp.float32)
    solution = jnp.zeros_like(right_side)
    residual = right_side
    for restart in range(ITERS):
        vectors, images = chebyshev(residual, diagonal)
        matrix = sketch(images + [residual], signs, table_x, table_y, table_z)
        weights_solved = least_squares(matrix)
        for position in range(BASIS):
            solution = solution + weights_solved[position] * vectors[position]
            residual = residual - weights_solved[position] * images[position]
    return (solution, residual)
```

```python
import jax
import jax.numpy as jnp
from jax import lax
from jax.experimental import pallas as pl
from jax.experimental.pallas import tpu as pltpu
from jax.sharding import Mesh
from jax.sharding import PartitionSpec as P

BASIS = 8
DEGREE = 2 * BASIS
NX, NY, NZ, SKETCH = 32, 128, 1024, 2048
GX, GZ = 8, 8
SHARE = SKETCH // GX
GY = ("gy_0", "gy_1")
tiny_value = 1e-06
VMEM = pltpu.VMEM
f32, bf16 = jnp.float32, jnp.bfloat16


def shifted(value, axis_name, size, by):
    pairs = [(i, i + by) for i in range(size) if 0 <= i + by < size]
    return lax.ppermute(value, axis_name, pairs)


def cosine_table(freqs, offset, count, length):
    indices = offset + jnp.arange(count, dtype=jnp.int32)
    phases = (2 * indices[:, None] + 1) * freqs[None, :] % (4 * length)
    return (jnp.sqrt(2.0 / length) * jnp.cos(jnp.pi * phases / (2.0 * length))).astype(f32)


def split_3(value):
    high = value.astype(bf16)
    rest = value - high.astype(f32)
    middle = rest.astype(bf16)
    low = (rest - middle.astype(f32)).astype(bf16)
    return high, middle, low


def around(field, value):
    rows, lanes = value.shape
    beside = pltpu.roll(value, 1, 0) + pltpu.roll(value, rows - 1, 0)
    return field + beside + (pltpu.roll(value, 1, 1) + pltpu.roll(value, lanes - 1, 1))


def basis_kernel(at_ref, mid_ref, ym2_ref, ym1_ref, yp1_ref, yp2_ref, t1_ref, t2_ref, t3_ref, w_ref,
                 part_ref, kept_ref, ka_ref, kb_ref, even, odd, coef, lhs):
    gx, gy, gz = at_ref[0], at_ref[1], at_ref[2]
    row = lax.broadcasted_iota(jnp.int32, (40, 256), 0) - 16 + gy * 8
    lane = lax.broadcasted_iota(jnp.int32, (40, 256), 1)
    used = (lane < 144) | (lane >= 240)
    place = jnp.where(lane >= 192, lane - 256, lane) + gz * 128
    inside = used & (row >= 0) & (row < NY) & (place >= 0) & (place < NZ)
    b_full = jnp.where(inside, 2.0 / 7.0, 0.0).astype(f32)
    lane8 = lax.broadcasted_iota(jnp.int32, (8, 128), 1)
    tail_used = (lane8 < 16) | (lane8 >= 112)
    zero_plane = jnp.zeros((40, 256), f32)
    for ref in (even, odd):
        ref[0] = zero_plane
        ref[NX + 1] = zero_plane

    def fill(x, carry):
        chip, k = x // 4, x % 4
        amount = 112 - 32 * k
        for n, ref in enumerate((ym2_ref, ym1_ref, mid_ref, yp1_ref, yp2_ref)):
            rows = pl.ds(8 * n, 8)
            inner = b_full[8 * n:8 * n + 8]
            tail = pltpu.roll(ref[chip, 8], amount, 1)
            even[x + 1, rows, 0:128] = ref[chip, k]
            even[x + 1, rows, 128:256] = jnp.where(tail_used, tail, 0.0)
            tail = pltpu.roll(ref[chip, 9], amount, 1)
            coef[x, rows, 0:128] = (ref[chip, 4 + k] - 1.0) * inner[:, 0:128]
            coef[x, rows, 128:256] = (tail - 1.0) * inner[:, 128:256]
        return carry

    lax.fori_loop(0, NX, fill, 0)

    def put(pair, first, second):
        chip, k = pair // 2, 2 * (pair % 2)
        block = jnp.concatenate([first * mid_ref[chip, 10 + k], second * mid_ref[chip, 11 + k]], axis=0)
        high, middle, low = split_3(block)
        rows = pl.ds(pl.multiple_of(pair * 16, 16), 16)
        lhs[rows, 0:128] = middle
        lhs[rows, 128:256] = high
        lhs[rows, 256:384] = low

    def project(m):
        total = jnp.dot(lhs[:, 0:256], t1_ref[...], preferred_element_type=f32)
        total += jnp.dot(lhs[:, 0:256], t2_ref[...], preferred_element_type=f32)
        total += jnp.dot(lhs[:, 128:384], t3_ref[...], preferred_element_type=f32)
        part_ref[m:m + 1, :] = jnp.sum(total * w_ref[...], axis=0, keepdims=True)

    def keep(m, ref):
        def one(p, carry):
            plane = jnp.clip(4 * gx - 7 + p, 0, NX + 1)
            kept_ref[m, p] = ref[plane, 8:32, :]
            return carry
        lax.fori_loop(0, 20, one, 0)

    def keep_coef(p, carry):
        x = 4 * gx - 8 + p
        real = ((x >= 0) & (x < NX)).astype(f32)
        ka_ref[p] = coef[jnp.clip(x, 0, NX - 1), 8:32, :] * real
        kb_ref[p] = b_full[8:32] * real
        return carry

    lax.fori_loop(0, 20, keep_coef, 0)

    def first_put(pair, carry):
        put(pair, even[2 * pair + 1, 16:24, 0:128], even[2 * pair + 2, 16:24, 0:128])
        return carry

    lax.fori_loop(0, NX // 2, first_put, 0)
    project(0)
    keep(0, even)
    now, other = even, odd
    for m in range(1, DEGREE + 1):
        low, high = (0, 40) if m <= BASIS else (8, 32)
        own = slice(16 - low, 24 - low)
        b = b_full[low:high]

        def step(pair, carry, m=m, low=low, high=high, own=own, b=b, now=now, other=other):
            x = 2 * pair
            p0, p1, p2, p3 = [now[x + k, low:high, :] for k in range(4)]
            results = []
            for k, (before, here, after) in enumerate(((p0, p1, p2), (p1, p2, p3))):
                beside = around(before + after, here)
                value = coef[x + k, low:high, :] * here - b * beside
                value = 0.5 * value if m == 1 else value - other[x + k + 1, low:high, :]
                other[x + k + 1, low:high, :] = value
                results.append(value[own, 0:128])
            put(pair, *results)
            return carry

        lax.fori_loop(0, NX // 2, step, 0)
        project(m)
        if m <= BASIS:
            keep(m, other)
        now, other = other, now


def total_of(value):
    return jnp.sum(jnp.sum(value, axis=0, keepdims=True), axis=1, keepdims=True)


def dot_of(left, right):
    product = left * right
    half = product.shape[1] // 2
    return total_of(product[:, :half] + product[:, half:])


def images_of(vectors):
    out = [7.0 * (vectors[0] + vectors[1])]
    for k in range(1, BASIS):
        out.append(7.0 * vectors[k] + 3.5 * (vectors[k + 1] + vectors[k - 1]))
    return out


def solve(columns, target):
    columns = list(columns)
    basis, upper, overlap, inverse = [], {}, {}, []
    for j in range(BASIS):
        column = columns[j]
        if j:
            seen = [dot_of(basis[i], column) for i in range(j)]
            amounts = []
            for i in range(j):
                amount = seen[i]
                for k in range(i):
                    amount = amount - amounts[k] * overlap[i, k]
                amounts.append(amount)
            for i in range(j):
                column = column - amounts[i] * basis[i]
                upper[i, j] = upper[i, j] + amounts[i]
        length = jnp.sqrt(dot_of(column, column) + tiny_value)
        inverse.append(1.0 / length)
        basis.append(column * inverse[j])
        for later in range(j + 1, BASIS):
            amount = dot_of(basis[j], columns[later])
            columns[later] = columns[later] - amount * basis[j]
            upper[j, later] = amount
        for k in range(j):
            overlap[j, k] = dot_of(basis[j], basis[k])
    solved = [dot_of(vector, target) for vector in basis]
    for i in range(BASIS - 1, -1, -1):
        solved[i] = solved[i] * inverse[i]
        for k in range(i):
            solved[k] = solved[k] - upper[k, i] * solved[i]
    return solved


def remainder_of(solved):
    out = [-7.0 * c for c in solved] + [jnp.zeros_like(solved[0])]
    out[0] = out[0] + 1.0
    out[1] = out[1] - 7.0 * solved[0]
    for k in range(1, BASIS):
        out[k + 1] = out[k + 1] - 3.5 * solved[k]
        out[k - 1] = out[k - 1] - 3.5 * solved[k]
    return out


def finish_kernel(rows_ref, kept_ref, ka_ref, kb_ref, sol_ref, res_ref, even, odd):
    rows = [rows_ref[m] for m in range(DEGREE + 1)]
    first = solve(images_of(rows[:BASIS + 1]), rows[0])
    rest = remainder_of(first)
    turned = []
    for j in range(BASIS + 1):
        value = rest[0] * rows[j]
        for m in range(1, BASIS + 1):
            value = value + (0.5 * rest[m]) * (rows[m + j] + rows[abs(m - j)])
        turned.append(value)
    second = solve(images_of(turned), turned[0])
    last = remainder_of(second)

    zero_plane = jnp.zeros((24, 256), f32)
    for ref in (even, odd):
        ref[0] = zero_plane
        ref[21] = zero_plane

    def start(p, carry):
        value = rest[0] * kept_ref[0, p]
        for m in range(1, BASIS + 1):
            value = value + rest[m] * kept_ref[m, p]
        even[p + 1] = value
        return carry

    lax.fori_loop(0, 20, start, 0)
    for p in range(4):
        value = first[0] * kept_ref[0, 8 + p, 8:16, 0:128]
        for m in range(1, BASIS):
            value = value + first[m] * kept_ref[m, 8 + p, 8:16, 0:128]
        here = even[9 + p, 8:16, 0:128]
        sol_ref[p] = value + second[0] * here
        res_ref[p] = last[0] * here
    now, other = even, odd
    for m in range(1, BASIS + 1):
        def step(p, carry, m=m, now=now, other=other):
            here = now[p + 1]
            beside = around(now[p] + now[p + 2], here)
            value = ka_ref[p] * here - kb_ref[p] * beside
            other[p + 1] = 0.5 * value if m == 1 else value - other[p + 1]
            return carry

        lax.fori_loop(m, 20 - m, step, 0)
        for p in range(4):
            here = other[9 + p, 8:16, 0:128]
            if m < BASIS:
                sol_ref[p] += second[m] * here
            res_ref[p] += last[m] * here
        now, other = other, now


def run_basis(at, mid, sides, tables, weights, interpret=False):
    return pl.pallas_call(
        basis_kernel,
        out_shape=[
            jax.ShapeDtypeStruct((DEGREE + 1, SHARE), f32),
            jax.ShapeDtypeStruct((BASIS + 1, 20, 24, 256), f32),
            jax.ShapeDtypeStruct((20, 24, 256), f32),
            jax.ShapeDtypeStruct((20, 24, 256), f32),
        ],
        in_specs=[pl.BlockSpec(memory_space=pltpu.SMEM)] + [pl.BlockSpec(memory_space=VMEM)] * 9,
        out_specs=[pl.BlockSpec(memory_space=VMEM)] * 4,
        scratch_shapes=[
            VMEM((NX + 2, 40, 256), f32),
            VMEM((NX + 2, 40, 256), f32),
            VMEM((NX, 40, 256), f32),
            VMEM((256, 384), bf16),
        ],
        name="basis",
        interpret=interpret,
    )(at, mid, *sides, *tables, weights)


def run_finish(rows, kept, ka, kb, interpret=False):
    return pl.pallas_call(
        finish_kernel,
        out_shape=[jax.ShapeDtypeStruct((4, 8, 128), f32)] * 2,
        in_specs=[pl.BlockSpec(memory_space=VMEM)] * 4,
        out_specs=[pl.BlockSpec(memory_space=VMEM)] * 2,
        scratch_shapes=[VMEM((22, 24, 256), f32), VMEM((22, 24, 256), f32)],
        name="finish",
        interpret=interpret,
    )(rows, kept, ka, kb)


def prepared_tables(freq_x, freq_y, freq_z, gx, gy, gz):
    mine = [lax.dynamic_slice_in_dim(f, gx * SHARE, SHARE) for f in (freq_x, freq_y, freq_z)]
    table_x = cosine_table(mine[0], 0, NX, NX)
    table_y = cosine_table(mine[1], gy * 8, 8, NY)
    table_z = cosine_table(mine[2], gz * 128, 128, NZ)
    high, middle, low = split_3(table_z)
    tables = [jnp.concatenate(pair, axis=0) for pair in ((high, high), (middle, middle), (low, high))]
    weights = (table_x[:, None, :] * table_y[None, :, :]).reshape(NX * 8, SHARE)
    return tables, weights


def to_all(value, axis, size):
    return lax.all_to_all(
        jnp.broadcast_to(value[None], (size, *value.shape)), axis, 0, 0, tiled=True
    )


def tail_of(before, after):
    pieces = []
    for k in range(4):
        pieces += [before[:, k], after[:, k]]
    return jnp.concatenate(pieces, axis=-1)


def shards(right_side, diagonal, sign_bits, freq_x, freq_y, freq_z):
    gx, gy, gz = lax.axis_index("gx"), lax.axis_index(GY), lax.axis_index("gz")
    both = jnp.stack([right_side, diagonal])
    before = shifted(both[..., -16:], "gz", GZ, 1)
    after = shifted(both[..., :16], "gz", GZ, -1)
    signs = 1.0 - 2.0 * sign_bits.astype(f32)
    sent = jnp.concatenate([both.reshape(8, 8, 128), tail_of(before, after), signs], axis=0)
    mid = to_all(sent, "gx", GX)
    shared = mid[:, :10]
    sides = [shifted(shared, GY, 16, by) for by in (2, 1, -1, -2)]
    tables, weights = prepared_tables(freq_x, freq_y, freq_z, gx, gy, gz)
    at = jnp.stack([gx, gy, gz]).astype(jnp.int32)
    part, kept, ka, kb = run_basis(at, mid, sides, tables, weights)
    rows = reduced(part)
    return tuple(run_finish(rows, kept, ka, kb))


def reduced(part):
    pieces = part.reshape(17, GZ, 32).transpose(1, 0, 2).reshape(GZ, 544)
    pieces = lax.all_to_all(pieces, "gz", 0, 0, tiled=True).sum(axis=0)
    pieces = to_all(pieces, GY, 16).sum(axis=0)
    pieces = to_all(pieces, ("gx", "gz"), GX * GZ)
    return pieces.reshape(8, 8, 17, 32).transpose(2, 0, 1, 3).reshape(17, 8, 256)


def solution(mesh):
    split = Mesh(
        mesh.devices.reshape(mesh.shape["gx"], 8, 2, mesh.shape["gz"]), ("gx", "gy_0", "gy_1", "gz")
    )
    return jax.shard_map(
        shards,
        mesh=split,
        in_specs=(P("gx", GY, "gz"), P("gx", GY, "gz"), P("gx", GY, "gz"), P(), P(), P()),
        out_specs=(P("gx", GY, "gz"), P("gx", GY, "gz")),
        check_vma=False,
    )
```

```python
import jax
import jax.numpy as jnp
from jax import lax
from jax.experimental import pallas as pl
from jax.experimental.pallas import tpu as pltpu
from jax.sharding import Mesh
from jax.sharding import PartitionSpec as P

BASIS = 8
DEGREE = 2 * BASIS
NX, NY, NZ, SKETCH = 32, 128, 1024, 2048
GX, GZ = 8, 8
SHARE = SKETCH // GX
GY = ("gy_0", "gy_1")
tiny_value = 1e-06
VMEM = pltpu.VMEM
f32, bf16 = jnp.float32, jnp.bfloat16


def shifted(value, axis_name, size, by):
    pairs = [(i, i + by) for i in range(size) if 0 <= i + by < size]
    return lax.ppermute(value, axis_name, pairs)


def cosine_table(freqs, offset, count, length):
    indices = offset + jnp.arange(count, dtype=jnp.int32)
    phases = (2 * indices[:, None] + 1) * freqs[None, :] % (4 * length)
    return (jnp.sqrt(2.0 / length) * jnp.cos(jnp.pi * phases / (2.0 * length))).astype(f32)


def split_3(value):
    high = value.astype(bf16)
    rest = value - high.astype(f32)
    middle = rest.astype(bf16)
    low = (rest - middle.astype(f32)).astype(bf16)
    return high, middle, low


def beside_z(halves):
    lane = lax.broadcasted_iota(jnp.int32, halves[0].shape, 1)
    low = [pltpu.roll(half, 1, 1) for half in halves]
    high = [pltpu.roll(half, 127, 1) for half in halves]
    return [
        jnp.where(lane == 0, low[1 - h], low[h]) + jnp.where(lane == 127, high[1 - h], high[h])
        for h in range(2)
    ]


def next_plane(now, other, coef, scale, x, rows, first, at=None):
    low, high = rows
    at = x if at is None else at
    here = [now[x + 1, h, low:high, :] for h in range(2)]
    sides = beside_z(here)
    out = []
    for h in range(2):
        total = now[x, h, low:high, :] + now[x + 2, h, low:high, :]
        total = total + (now[x + 1, h, low - 1:high - 1, :] + now[x + 1, h, low + 1:high + 1, :])
        total = total + sides[h]
        value = coef[at, h, low - 8:high - 8, :] * here[h] - scale(h) * total
        value = 0.5 * value if first else value - other[x + 1, h, low:high, :]
        other[x + 1, h, low:high, :] = value
        out.append(value)
    return out


def basis_kernel(at_ref, mid_ref, ym2_ref, ym1_ref, yp1_ref, yp2_ref, table_ref, w_ref,
                 part_ref, kept_ref, ka_ref, kb_ref, even, odd, coef, mask, lhs):
    gx, gy, gz = at_ref[0], at_ref[1], at_ref[2]
    row = lax.broadcasted_iota(jnp.int32, (40, 128), 0) - 16 + gy * 8
    lane = lax.broadcasted_iota(jnp.int32, (40, 128), 1)
    rows_in = (row >= 0) & (row < NY)
    mask[0] = jnp.where(rows_in, 2.0 / 7.0, 0.0).astype(f32)
    place = jnp.where(lane >= 64, lane - 128, lane + 128) + gz * 128
    tail_in = rows_in & ((lane < 16) | (lane >= 112)) & (place >= 0) & (place < NZ)
    mask[1] = jnp.where(tail_in, 2.0 / 7.0, 0.0).astype(f32)
    lane8 = lax.broadcasted_iota(jnp.int32, (8, 128), 1)
    tail_used = (lane8 < 16) | (lane8 >= 112)
    empty = jnp.zeros((8, 128), f32)
    for ref in (even, odd):
        for plane in (0, NX + 1):
            for h in range(2):
                ref[plane, h] = jnp.zeros((56, 128), f32)

    def fill(chip, carry):
        for k in range(4):
            x = 4 * chip + k
            for h in range(2):
                for ref in (even, odd):
                    ref[x + 1, h, 0:8, :] = empty
                    ref[x + 1, h, 48:56, :] = empty
            for n, ref in enumerate((ym2_ref, ym1_ref, mid_ref, yp1_ref, yp2_ref)):
                rows = slice(8 * n, 8 * n + 8)
                padded = slice(8 * n + 8, 8 * n + 16)
                even[x + 1, 0, padded, :] = ref[chip, k]
                tail = pltpu.roll(ref[chip, 8], 112 - 32 * k, 1)
                even[x + 1, 1, padded, :] = jnp.where(tail_used, tail, 0.0)
                coef[x, 0, rows, :] = (ref[chip, 4 + k] - 1.0) * mask[0, rows, :]
                tail = pltpu.roll(ref[chip, 9], 112 - 32 * k, 1)
                coef[x, 1, rows, :] = (tail - 1.0) * mask[1, rows, :]
        return carry

    lax.fori_loop(0, GX, fill, 0)

    def put(m, chip, k, first, second):
        block = jnp.concatenate([first * mid_ref[chip, 10 + k], second * mid_ref[chip, 11 + k]], axis=0)
        high, middle, low = split_3(block)
        rows = pl.ds(pl.multiple_of(256 * (m % 2) + 32 * chip + 8 * k, 16), 16)
        lhs[rows, 0:128] = middle
        lhs[rows, 128:256] = high
        lhs[rows, 256:384] = low

    def project(begin, end):
        size = 256 * (end - begin)
        rows = lhs[0:size, :]
        stacked = jnp.concatenate([rows[:, 0:256], rows[:, 0:256], rows[:, 128:384]], axis=1)
        total = jnp.dot(stacked, table_ref[...], preferred_element_type=f32)
        for m in range(begin, end):
            own = total[256 * (m - begin):256 * (m - begin + 1)]
            part_ref[m:m + 1, :] = jnp.sum(own * w_ref[...], axis=0, keepdims=True)

    def keep(m, ref):
        def one(p, carry):
            plane = jnp.clip(4 * gx - 7 + p, 0, NX + 1)
            kept_ref[m, p] = ref[plane, :, 16:40, :]
            return carry
        lax.fori_loop(0, 20, one, 0, unroll=4)

    def keep_coef(p, carry):
        x = 4 * gx - 8 + p
        real = ((x >= 0) & (x < NX)).astype(f32)
        ka_ref[p] = coef[jnp.clip(x, 0, NX - 1), :, 8:32, :] * real
        kb_ref[p] = mask[:, 8:32, :] * real
        return carry

    lax.fori_loop(0, 20, keep_coef, 0)

    def first_put(chip, carry):
        for k in (0, 2):
            put(0, chip, k, *[even[4 * chip + k + d + 1, 0, 24:32, :] for d in range(2)])
        return carry

    lax.fori_loop(0, GX, first_put, 0)
    keep(0, even)
    now, other = even, odd
    for m in range(1, DEGREE + 1):
        rows = (8, 48) if m <= BASIS else (16, 40)

        def step(chip, carry, m=m, rows=rows, now=now, other=other):
            own = slice(24 - rows[0], 32 - rows[0])
            for k in (0, 2):
                pair = []
                for d in range(2):
                    x = 4 * chip + k + d
                    scale = lambda h: mask[h, rows[0] - 8:rows[1] - 8, :]
                    pair.append(next_plane(now, other, coef, scale, x, rows, m == 1)[0][own])
                put(m, chip, k, *pair)
            return carry

        lax.fori_loop(0, GX, step, 0)
        if m % 2:
            project(m - 1, m + 1)
        if m <= BASIS:
            keep(m, other)
        now, other = other, now
    project(DEGREE, DEGREE + 1)


def total_of(value):
    return jnp.sum(jnp.sum(value, axis=0, keepdims=True), axis=1, keepdims=True)


def dot_of(left, right):
    product = left * right
    half = product.shape[1] // 2
    return total_of(product[:, :half] + product[:, half:])


def images_of(vectors):
    out = [7.0 * (vectors[0] + vectors[1])]
    for k in range(1, BASIS):
        out.append(7.0 * vectors[k] + 3.5 * (vectors[k + 1] + vectors[k - 1]))
    return out


def solve(columns, target):
    columns = list(columns)
    basis, upper, overlap, inverse = [], {}, {}, []
    for j in range(BASIS):
        column = columns[j]
        if j:
            seen = [dot_of(basis[i], column) for i in range(j)]
            amounts = []
            for i in range(j):
                amount = seen[i]
                for k in range(i):
                    amount = amount - amounts[k] * overlap[i, k]
                amounts.append(amount)
            for i in range(j):
                column = column - amounts[i] * basis[i]
                upper[i, j] = upper[i, j] + amounts[i]
        length = jnp.sqrt(dot_of(column, column) + tiny_value)
        inverse.append(1.0 / length)
        basis.append(column * inverse[j])
        for later in range(j + 1, BASIS):
            amount = dot_of(basis[j], columns[later])
            columns[later] = columns[later] - amount * basis[j]
            upper[j, later] = amount
        for k in range(j):
            overlap[j, k] = dot_of(basis[j], basis[k])
    solved = [dot_of(vector, target) for vector in basis]
    for i in range(BASIS - 1, -1, -1):
        solved[i] = solved[i] * inverse[i]
        for k in range(i):
            solved[k] = solved[k] - upper[k, i] * solved[i]
    return solved


def remainder_of(solved):
    out = [-7.0 * c for c in solved] + [jnp.zeros_like(solved[0])]
    out[0] = out[0] + 1.0
    out[1] = out[1] - 7.0 * solved[0]
    for k in range(1, BASIS):
        out[k + 1] = out[k + 1] - 3.5 * solved[k]
        out[k - 1] = out[k - 1] - 3.5 * solved[k]
    return out


def finish_kernel(rows_ref, kept_ref, ka_ref, kb_ref, sol_ref, res_ref, even, odd):
    rows = [rows_ref[m] for m in range(DEGREE + 1)]
    first = solve(images_of(rows[:BASIS + 1]), rows[0])
    rest = remainder_of(first)
    turned = []
    for j in range(BASIS + 1):
        value = rest[0] * rows[j]
        for m in range(1, BASIS + 1):
            value = value + (0.5 * rest[m]) * (rows[m + j] + rows[abs(m - j)])
        turned.append(value)
    second = solve(images_of(turned), turned[0])
    last = remainder_of(second)

    for ref in (even, odd):
        for h in range(2):
            ref[0, h] = jnp.zeros((40, 128), f32)
            ref[21, h] = jnp.zeros((40, 128), f32)

    def start(p, carry):
        for h in range(2):
            value = rest[0] * kept_ref[0, p, h]
            for m in range(1, BASIS + 1):
                value = value + rest[m] * kept_ref[m, p, h]
            even[p + 1, h, 8:32, :] = value
            for ref in (even, odd):
                ref[p + 1, h, 0:8, :] = jnp.zeros((8, 128), f32)
                ref[p + 1, h, 32:40, :] = jnp.zeros((8, 128), f32)
        return carry

    lax.fori_loop(0, 20, start, 0)
    for p in range(4):
        value = first[0] * kept_ref[0, 8 + p, 0, 8:16, :]
        for m in range(1, BASIS):
            value = value + first[m] * kept_ref[m, 8 + p, 0, 8:16, :]
        here = even[9 + p, 0, 16:24, :]
        sol_ref[p] = value + second[0] * here
        res_ref[p] = last[0] * here
    now, other = even, odd
    for m in range(1, BASIS + 1):
        def step(q, carry, m=m, now=now, other=other):
            for d in range(2):
                p = m + 2 * q + d
                scale = lambda h: kb_ref[p, h]
                next_plane(now, other, ka_ref, scale, p, (8, 32), m == 1)
            return carry

        lax.fori_loop(0, 10 - m, step, 0)
        for p in range(4):
            here = other[9 + p, 0, 16:24, :]
            if m < BASIS:
                sol_ref[p] += second[m] * here
            res_ref[p] += last[m] * here
        now, other = other, now


def run_basis(at, mid, sides, table, weights, interpret=False):
    return pl.pallas_call(
        basis_kernel,
        out_shape=[
            jax.ShapeDtypeStruct((DEGREE + 1, SHARE), f32),
            jax.ShapeDtypeStruct((BASIS + 1, 20, 2, 24, 128), f32),
            jax.ShapeDtypeStruct((20, 2, 24, 128), f32),
            jax.ShapeDtypeStruct((20, 2, 24, 128), f32),
        ],
        in_specs=[pl.BlockSpec(memory_space=pltpu.SMEM)] + [pl.BlockSpec(memory_space=VMEM)] * 7,
        out_specs=[pl.BlockSpec(memory_space=VMEM)] * 4,
        scratch_shapes=[
            VMEM((NX + 2, 2, 56, 128), f32),
            VMEM((NX + 2, 2, 56, 128), f32),
            VMEM((NX, 2, 40, 128), f32),
            VMEM((2, 40, 128), f32),
            VMEM((512, 384), bf16),
        ],
        compiler_params=pltpu.CompilerParams(vmem_limit_bytes=28 << 20),
        name="basis",
        interpret=interpret,
    )(at, mid, *sides, table, weights)


def run_finish(rows, kept, ka, kb, interpret=False):
    return pl.pallas_call(
        finish_kernel,
        out_shape=[jax.ShapeDtypeStruct((4, 8, 128), f32)] * 2,
        in_specs=[pl.BlockSpec(memory_space=VMEM)] * 4,
        out_specs=[pl.BlockSpec(memory_space=VMEM)] * 2,
        scratch_shapes=[VMEM((22, 2, 40, 128), f32), VMEM((22, 2, 40, 128), f32)],
        compiler_params=pltpu.CompilerParams(vmem_limit_bytes=28 << 20),
        name="finish",
        interpret=interpret,
    )(rows, kept, ka, kb)


def prepared_tables(freq_x, freq_y, freq_z, gx, gy, gz):
    mine = [lax.dynamic_slice_in_dim(f, gx * SHARE, SHARE) for f in (freq_x, freq_y, freq_z)]
    table_x = cosine_table(mine[0], 0, NX, NX)
    table_y = cosine_table(mine[1], gy * 8, 8, NY)
    table_z = cosine_table(mine[2], gz * 128, 128, NZ)
    high, middle, low = split_3(table_z)
    table = jnp.concatenate([high, high, middle, middle, low, high], axis=0)
    weights = (table_x[:, None, :] * table_y[None, :, :]).reshape(NX * 8, SHARE)
    return table, weights


def to_all(value, axis, size):
    return lax.all_to_all(
        jnp.broadcast_to(value[None], (size, *value.shape)), axis, 0, 0, tiled=True
    )


def tail_of(before, after):
    pieces = []
    for k in range(4):
        pieces += [before[:, k], after[:, k]]
    return jnp.concatenate(pieces, axis=-1)


def shards(right_side, diagonal, sign_bits, freq_x, freq_y, freq_z):
    gx, gy, gz = lax.axis_index("gx"), lax.axis_index(GY), lax.axis_index("gz")
    both = jnp.stack([right_side, diagonal])
    before = shifted(both[..., -16:], "gz", GZ, 1)
    after = shifted(both[..., :16], "gz", GZ, -1)
    signs = 1.0 - 2.0 * sign_bits.astype(f32)
    sent = jnp.concatenate([both.reshape(8, 8, 128), tail_of(before, after), signs], axis=0)
    mid = to_all(sent, "gx", GX)
    shared = mid[:, :10]
    sides = [shifted(shared, GY, 16, by) for by in (2, 1, -1, -2)]
    table, weights = prepared_tables(freq_x, freq_y, freq_z, gx, gy, gz)
    at = jnp.stack([gx, gy, gz]).astype(jnp.int32)
    part, kept, ka, kb = run_basis(at, mid, sides, table, weights)
    rows = reduced(part)
    return tuple(run_finish(rows, kept, ka, kb))


def reduced(part):
    pieces = part.reshape(17, GZ, 32).transpose(1, 0, 2).reshape(GZ, 544)
    pieces = lax.all_to_all(pieces, "gz", 0, 0, tiled=True).sum(axis=0)
    pieces = to_all(pieces, GY, 16).sum(axis=0)
    pieces = to_all(pieces, ("gx", "gz"), GX * GZ)
    return pieces.reshape(8, 8, 17, 32).transpose(2, 0, 1, 3).reshape(17, 8, 256)


def solution(mesh):
    split = Mesh(
        mesh.devices.reshape(mesh.shape["gx"], 8, 2, mesh.shape["gz"]), ("gx", "gy_0", "gy_1", "gz")
    )
    return jax.shard_map(
        shards,
        mesh=split,
        in_specs=(P("gx", GY, "gz"), P("gx", GY, "gz"), P("gx", GY, "gz"), P(), P(), P()),
        out_specs=(P("gx", GY, "gz"), P("gx", GY, "gz")),
        check_vma=False,
    )
```

```python
import jax
import jax.numpy as jnp
from jax import lax
from jax.experimental import pallas as pl
from jax.experimental.pallas import tpu as pltpu
from jax.sharding import Mesh
from jax.sharding import PartitionSpec as P

BASIS = 8
DEGREE = 2 * BASIS
NX, NY, NZ, SKETCH = 32, 128, 1024, 2048
GX, GZ = 8, 8
SHARE = SKETCH // GX
GY = ("gy_0", "gy_1")
tiny_value = 1e-06
VMEM = pltpu.VMEM
f32, bf16 = jnp.float32, jnp.bfloat16


def shifted(value, axis_name, size, by):
    pairs = [(i, i + by) for i in range(size) if 0 <= i + by < size]
    return lax.ppermute(value, axis_name, pairs)


def cosine_table(freqs, offset, count, length):
    indices = offset + jnp.arange(count, dtype=jnp.int32)
    phases = (2 * indices[:, None] + 1) * freqs[None, :] % (4 * length)
    return (jnp.sqrt(2.0 / length) * jnp.cos(jnp.pi * phases / (2.0 * length))).astype(f32)


def split_3(value):
    high = value.astype(bf16)
    rest = value - high.astype(f32)
    middle = rest.astype(bf16)
    low = (rest - middle.astype(f32)).astype(bf16)
    return high, middle, low


def beside_z(halves):
    lane = lax.broadcasted_iota(jnp.int32, halves[0].shape, 1)
    low = [pltpu.roll(half, 1, 1) for half in halves]
    high = [pltpu.roll(half, 127, 1) for half in halves]
    return [
        jnp.where(lane == 0, low[1 - h], low[h]) + jnp.where(lane == 127, high[1 - h], high[h])
        for h in range(2)
    ]


def halves_of(field, x, rows):
    return [field[x + 1, h, rows[0]:rows[1], :] for h in range(2)]


def next_plane(now, other, coef, scale, x, rows, first, sides):
    low, high = rows
    here = halves_of(now, x, rows)
    out = []
    for h in range(2):
        total = now[x, h, low:high, :] + now[x + 2, h, low:high, :]
        total = total + (now[x + 1, h, low - 1:high - 1, :] + now[x + 1, h, low + 1:high + 1, :])
        total = total + sides[h]
        value = coef[x, h, low - 8:high - 8, :] * here[h] - scale(h) * total
        value = 0.5 * value if first else value - other[x + 1, h, low:high, :]
        other[x + 1, h, low:high, :] = value
        out.append(value)
    return out


def basis_kernel(at_ref, mid_ref, ym2_ref, ym1_ref, yp1_ref, yp2_ref, table_ref, w_ref,
                 part_ref, kept_ref, ka_ref, kb_ref, even, odd, coef, mask, lhs):
    gx, gy, gz = at_ref[0], at_ref[1], at_ref[2]
    row = lax.broadcasted_iota(jnp.int32, (40, 128), 0) - 16 + gy * 8
    lane = lax.broadcasted_iota(jnp.int32, (40, 128), 1)
    rows_in = (row >= 0) & (row < NY)
    mask[0] = jnp.where(rows_in, 2.0 / 7.0, 0.0).astype(f32)
    place = jnp.where(lane >= 64, lane - 128, lane + 128) + gz * 128
    tail_in = rows_in & ((lane < 16) | (lane >= 112)) & (place >= 0) & (place < NZ)
    mask[1] = jnp.where(tail_in, 2.0 / 7.0, 0.0).astype(f32)
    lane8 = lax.broadcasted_iota(jnp.int32, (8, 128), 1)
    tail_used = (lane8 < 16) | (lane8 >= 112)
    empty = jnp.zeros((8, 128), f32)
    for m in range(DEGREE + 1, 3 * GZ):
        part_ref[m // 3, m % 3:m % 3 + 1, :] = jnp.zeros((1, SHARE), f32)
    for ref in (even, odd):
        for plane in (0, NX + 1):
            for h in range(2):
                ref[plane, h] = jnp.zeros((56, 128), f32)

    def fill(chip, carry):
        for k in range(4):
            x = 4 * chip + k
            for h in range(2):
                for ref in (even, odd):
                    ref[x + 1, h, 0:8, :] = empty
                    ref[x + 1, h, 48:56, :] = empty
            for n, ref in enumerate((ym2_ref, ym1_ref, mid_ref, yp1_ref, yp2_ref)):
                rows = slice(8 * n, 8 * n + 8)
                padded = slice(8 * n + 8, 8 * n + 16)
                even[x + 1, 0, padded, :] = ref[chip, k]
                tail = pltpu.roll(ref[chip, 8], 112 - 32 * k, 1)
                even[x + 1, 1, padded, :] = jnp.where(tail_used, tail, 0.0)
                coef[x, 0, rows, :] = (ref[chip, 4 + k] - 1.0) * mask[0, rows, :]
                tail = pltpu.roll(ref[chip, 9], 112 - 32 * k, 1)
                coef[x, 1, rows, :] = (tail - 1.0) * mask[1, rows, :]
        return carry

    for chip in range(GX):
        fill(chip, 0)

    def put(m, chip, k, first, second):
        block = jnp.concatenate([first * mid_ref[chip, 10 + k], second * mid_ref[chip, 11 + k]], axis=0)
        high, middle, low = split_3(block)
        rows = slice(256 * (m % 4) + 32 * chip + 8 * k, 256 * (m % 4) + 32 * chip + 8 * k + 16)
        lhs[rows, 0:128] = middle
        lhs[rows, 128:256] = high
        lhs[rows, 256:384] = low

    def project(begin, end):
        size = 256 * (end - begin)
        rows = lhs[0:size, :]
        stacked = jnp.concatenate([rows[:, 0:256], rows[:, 0:256], rows[:, 128:384]], axis=1)
        total = jnp.dot(stacked, table_ref[...], preferred_element_type=f32)
        for m in range(begin, end):
            own = total[256 * (m - begin):256 * (m - begin + 1)]
            part_ref[m // 3, m % 3:m % 3 + 1, :] = jnp.sum(own * w_ref[...], axis=0, keepdims=True)

    def keep(m, ref):
        def one(p, carry):
            plane = jnp.clip(4 * gx - 7 + p, 0, NX + 1)
            kept_ref[m, p] = ref[plane, :, 16:40, :]
            return carry
        for p in range(20):
            one(p, 0)

    def keep_coef(p, carry):
        x = 4 * gx - 8 + p
        real = ((x >= 0) & (x < NX)).astype(f32)
        ka_ref[p] = coef[jnp.clip(x, 0, NX - 1), :, 8:32, :] * real
        kb_ref[p] = mask[:, 8:32, :] * real
        return carry

    for p in range(20):
        keep_coef(p, 0)

    for x in range(0, NX, 2):
        put(0, x // 4, x % 4, even[x + 1, 0, 24:32, :], even[x + 2, 0, 24:32, :])
    keep(0, even)
    now, other = even, odd
    for m in range(1, DEGREE + 1):
        rows = (8, 48) if m <= BASIS else (16, 40)
        cut = slice(rows[0] - 8, rows[1] - 8)
        own = slice(24 - rows[0], 32 - rows[0])
        scale = lambda h: mask[h, cut, :]
        for x in range(0, NX, 2):
            pair = []
            for d in range(2):
                beside = beside_z(halves_of(now, x + d, rows))
                pair.append(next_plane(now, other, coef, scale, x + d, rows, m == 1, beside)[0][own])
            put(m, x // 4, x % 4, *pair)
        if m % 4 == 3:
            project(m - 3, m + 1)
        if m <= BASIS:
            keep(m, other)
        now, other = other, now
    project(DEGREE, DEGREE + 1)


def total_of(value):
    return jnp.sum(jnp.sum(value, axis=0, keepdims=True), axis=1, keepdims=True)


def dot_of(left, right):
    product = left * right
    half = product.shape[1] // 2
    return total_of(product[:, :half] + product[:, half:])


def images_of(vectors):
    out = [7.0 * (vectors[0] + vectors[1])]
    for k in range(1, BASIS):
        out.append(7.0 * vectors[k] + 3.5 * (vectors[k + 1] + vectors[k - 1]))
    return out


def solve(columns, target):
    columns = list(columns)
    basis, upper, overlap, inverse = [], {}, {}, []
    for j in range(BASIS):
        column = columns[j]
        square = dot_of(column, column)
        if j:
            seen = [dot_of(basis[i], column) for i in range(j)]
            amounts = []
            for i in range(j):
                amount = seen[i]
                for k in range(i):
                    amount = amount - amounts[k] * overlap[i, k]
                amounts.append(amount)
            for i in range(j):
                column = column - amounts[i] * basis[i]
                upper[i, j] = upper[i, j] + amounts[i]
                spread = overlap[i, i] * amounts[i] - 2.0 * seen[i]
                for k in range(i):
                    spread = spread + (2.0 * overlap[i, k]) * amounts[k]
                square = square + spread * amounts[i]
        length = jnp.sqrt(jnp.maximum(square, 0.0) + tiny_value)
        inverse.append(1.0 / length)
        basis.append(column * inverse[j])
        for later in range(j + 1, BASIS):
            amount = dot_of(basis[j], columns[later])
            columns[later] = columns[later] - amount * basis[j]
            upper[j, later] = amount
        for k in range(j + 1):
            overlap[j, k] = dot_of(basis[j], basis[k])
    solved = [dot_of(vector, target) for vector in basis]
    for i in range(BASIS - 1, -1, -1):
        solved[i] = solved[i] * inverse[i]
        for k in range(i):
            solved[k] = solved[k] - upper[k, i] * solved[i]
    return solved


def remainder_of(solved):
    out = [-7.0 * c for c in solved] + [jnp.zeros_like(solved[0])]
    out[0] = out[0] + 1.0
    out[1] = out[1] - 7.0 * solved[0]
    for k in range(1, BASIS):
        out[k + 1] = out[k + 1] - 3.5 * solved[k]
        out[k - 1] = out[k - 1] - 3.5 * solved[k]
    return out


def finish_kernel(rows_ref, kept_ref, ka_ref, kb_ref, sol_ref, res_ref, even, odd):
    rows = []
    for m in range(DEGREE + 1):
        rows.append(jnp.concatenate(
            [rows_ref[GZ * chip + m // 3, m % 3:m % 3 + 1, :] for chip in range(GX)], axis=0
        ))
    for ref in (even, odd):
        for p in range(1, 21):
            for h in range(2):
                ref[p, h, 0:8, :] = jnp.zeros((8, 128), f32)
                ref[p, h, 32:40, :] = jnp.zeros((8, 128), f32)
    first = solve(images_of(rows[:BASIS + 1]), rows[0])
    rest = remainder_of(first)
    for p in range(20):
        for h in range(2):
            value = rest[0] * kept_ref[0, p, h]
            for m in range(1, BASIS + 1):
                value = value + rest[m] * kept_ref[m, p, h]
            even[p + 1, h, 8:32, :] = value
    turned = []
    for j in range(BASIS + 1):
        value = rest[0] * rows[j]
        for m in range(1, BASIS + 1):
            value = value + (0.5 * rest[m]) * (rows[m + j] + rows[abs(m - j)])
        turned.append(value)
    fields = [[even[9 + p, 0, 16:24, :] for p in range(4)]]
    now, other = even, odd
    for m in range(1, BASIS + 1):
        fields.append([])
        for p in range(m, 20 - m):
            sides = beside_z(halves_of(now, p, (8, 32)))
            value = next_plane(now, other, ka_ref, lambda h: kb_ref[p, h], p, (8, 32), m == 1, sides)
            if 8 <= p < 12:
                fields[m].append(value[0][8:16])
        now, other = other, now
    second = solve(images_of(turned), turned[0])
    last = remainder_of(second)
    for p in range(4):
        value = first[0] * kept_ref[0, 8 + p, 0, 8:16, :]
        for m in range(1, BASIS):
            value = value + first[m] * kept_ref[m, 8 + p, 0, 8:16, :]
        for m in range(BASIS):
            value = value + second[m] * fields[m][p]
        sol_ref[p] = value
        value = last[0] * fields[0][p]
        for m in range(1, BASIS + 1):
            value = value + last[m] * fields[m][p]
        res_ref[p] = value


def run_basis(at, mid, sides, table, weights, interpret=False):
    return pl.pallas_call(
        basis_kernel,
        out_shape=[
            jax.ShapeDtypeStruct((GZ, 3, SHARE), f32),
            jax.ShapeDtypeStruct((BASIS + 1, 20, 2, 24, 128), f32),
            jax.ShapeDtypeStruct((20, 2, 24, 128), f32),
            jax.ShapeDtypeStruct((20, 2, 24, 128), f32),
        ],
        in_specs=[pl.BlockSpec(memory_space=pltpu.SMEM)] + [pl.BlockSpec(memory_space=VMEM)] * 7,
        out_specs=[pl.BlockSpec(memory_space=VMEM)] * 4,
        scratch_shapes=[
            VMEM((NX + 2, 2, 56, 128), f32),
            VMEM((NX + 2, 2, 56, 128), f32),
            VMEM((NX, 2, 40, 128), f32),
            VMEM((2, 40, 128), f32),
            VMEM((1024, 384), bf16),
        ],
        compiler_params=pltpu.CompilerParams(vmem_limit_bytes=28 << 20),
        name="basis",
        interpret=interpret,
    )(at, mid, *sides, table, weights)


def run_finish(rows, kept, ka, kb, interpret=False):
    return pl.pallas_call(
        finish_kernel,
        out_shape=[jax.ShapeDtypeStruct((4, 8, 128), f32)] * 2,
        in_specs=[pl.BlockSpec(memory_space=VMEM)] * 4,
        out_specs=[pl.BlockSpec(memory_space=VMEM)] * 2,
        scratch_shapes=[VMEM((22, 2, 40, 128), f32), VMEM((22, 2, 40, 128), f32)],
        compiler_params=pltpu.CompilerParams(vmem_limit_bytes=28 << 20),
        name="finish",
        interpret=interpret,
    )(rows, kept, ka, kb)


def prepared_tables(freq_x, freq_y, freq_z, gx, gy, gz):
    mine = [lax.dynamic_slice_in_dim(f, gx * SHARE, SHARE) for f in (freq_x, freq_y, freq_z)]
    table_x = cosine_table(mine[0], 0, NX, NX)
    table_y = cosine_table(mine[1], gy * 8, 8, NY)
    table_z = cosine_table(mine[2], gz * 128, 128, NZ)
    high, middle, low = split_3(table_z)
    table = jnp.concatenate([high, high, middle, middle, low, high], axis=0)
    weights = (table_x[:, None, :] * table_y[None, :, :]).reshape(NX * 8, SHARE)
    return table, weights


def to_all(value, axis, size):
    return lax.all_to_all(
        jnp.broadcast_to(value[None], (size, *value.shape)), axis, 0, 0, tiled=True
    )


def tail_of(before, after):
    pieces = []
    for k in range(4):
        pieces += [before[:, k], after[:, k]]
    return jnp.concatenate(pieces, axis=-1)


def shards(right_side, diagonal, sign_bits, freq_x, freq_y, freq_z):
    gx, gy, gz = lax.axis_index("gx"), lax.axis_index(GY), lax.axis_index("gz")
    both = jnp.stack([right_side, diagonal])
    before = shifted(both[..., -16:], "gz", GZ, 1)
    after = shifted(both[..., :16], "gz", GZ, -1)
    signs = 1.0 - 2.0 * sign_bits.astype(f32)
    sent = jnp.concatenate([both.reshape(8, 8, 128), tail_of(before, after), signs], axis=0)
    mid = to_all(sent, "gx", GX)
    shared = mid[:, :10]
    sides = [shifted(shared, GY, 16, by) for by in (2, 1, -1, -2)]
    freq_x, freq_y, freq_z, mid = lax.optimization_barrier((freq_x, freq_y, freq_z, mid))
    table, weights = prepared_tables(freq_x, freq_y, freq_z, gx, gy, gz)
    at = jnp.stack([gx, gy, gz]).astype(jnp.int32)
    part, kept, ka, kb = run_basis(at, mid, sides, table, weights)
    rows = reduced(part)
    return tuple(run_finish(rows, kept, ka, kb))


def reduced(part):
    pieces = lax.all_to_all(part, "gz", 0, 0, tiled=True).sum(axis=0)
    pieces = to_all(pieces, GY, 16).sum(axis=0)
    return to_all(pieces, ("gx", "gz"), GX * GZ)


def solution(mesh):
    split = Mesh(
        mesh.devices.reshape(mesh.shape["gx"], 8, 2, mesh.shape["gz"]), ("gx", "gy_0", "gy_1", "gz")
    )
    return jax.shard_map(
        shards,
        mesh=split,
        in_specs=(P("gx", GY, "gz"), P("gx", GY, "gz"), P("gx", GY, "gz"), P(), P(), P()),
        out_specs=(P("gx", GY, "gz"), P("gx", GY, "gz")),
        check_vma=False,
    )
```

```python
import jax
import jax.numpy as jnp
from jax import lax
from jax.experimental import pallas as pl
from jax.experimental.pallas import tpu as pltpu
from jax.sharding import Mesh
from jax.sharding import PartitionSpec as P

BASIS = 8
DEGREE = 2 * BASIS
NX, NY, NZ, SKETCH = 32, 128, 1024, 2048
GX, GZ = 8, 8
SHARE = SKETCH // GX
GY = ("gy_0", "gy_1")
tiny_value = 1e-06
VMEM = pltpu.VMEM
f32, bf16 = jnp.float32, jnp.bfloat16


def shifted(value, axis_name, size, by):
    pairs = [(i, i + by) for i in range(size) if 0 <= i + by < size]
    return lax.ppermute(value, axis_name, pairs)


def cosine_table(freqs, offset, count, length):
    indices = offset + jnp.arange(count, dtype=jnp.int32)
    phases = (2 * indices[:, None] + 1) * freqs[None, :] % (4 * length)
    return (jnp.sqrt(2.0 / length) * jnp.cos(jnp.pi * phases / (2.0 * length))).astype(f32)


def split_3(value):
    high = value.astype(bf16)
    rest = value - high.astype(f32)
    middle = rest.astype(bf16)
    low = (rest - middle.astype(f32)).astype(bf16)
    return high, middle, low


def beside_z(halves):
    lane = lax.broadcasted_iota(jnp.int32, halves[0].shape, 1)
    low = [pltpu.roll(half, 1, 1) for half in halves]
    high = [pltpu.roll(half, 127, 1) for half in halves]
    return [
        jnp.where(lane == 0, low[1 - h], low[h]) + jnp.where(lane == 127, high[1 - h], high[h])
        for h in range(2)
    ]


def halves_of(field, x, rows):
    return [field[x + 1, h, rows[0]:rows[1], :] for h in range(2)]


def next_plane(now, other, coef, scale, x, rows, first, sides):
    low, high = rows
    here = halves_of(now, x, rows)
    out = []
    for h in range(2):
        total = now[x, h, low:high, :] + now[x + 2, h, low:high, :]
        total = total + (now[x + 1, h, low - 1:high - 1, :] + now[x + 1, h, low + 1:high + 1, :])
        total = total + sides[h]
        value = coef[x, h, low - 8:high - 8, :] * here[h] - scale(h) * total
        value = 0.5 * value if first else value - other[x + 1, h, low:high, :]
        other[x + 1, h, low:high, :] = value
        out.append(value)
    return out


def basis_kernel(at_ref, mid_ref, ym2_ref, ym1_ref, yp1_ref, yp2_ref, table_ref, w_ref,
                 part_ref, kept_ref, ka_ref, kb_ref, even, odd, coef, mask, lhs, held, held_a, held_b, sems):
    gx, gy, gz = at_ref[0], at_ref[1], at_ref[2]
    row = lax.broadcasted_iota(jnp.int32, (40, 128), 0) - 16 + gy * 8
    lane = lax.broadcasted_iota(jnp.int32, (40, 128), 1)
    rows_in = (row >= 0) & (row < NY)
    mask[0] = jnp.where(rows_in, 2.0 / 7.0, 0.0).astype(f32)
    place = jnp.where(lane >= 64, lane - 128, lane + 128) + gz * 128
    tail_in = rows_in & ((lane < 16) | (lane >= 112)) & (place >= 0) & (place < NZ)
    mask[1] = jnp.where(tail_in, 2.0 / 7.0, 0.0).astype(f32)
    lane8 = lax.broadcasted_iota(jnp.int32, (8, 128), 1)
    tail_used = (lane8 < 16) | (lane8 >= 112)
    empty = jnp.zeros((8, 128), f32)
    for m in range(DEGREE + 1, 3 * GZ):
        part_ref[m // 3, m % 3:m % 3 + 1, :] = jnp.zeros((1, SHARE), f32)
    for ref in (even, odd):
        for plane in (0, NX + 1):
            for h in range(2):
                ref[plane, h] = jnp.zeros((56, 128), f32)

    def fill(chip, carry):
        for k in range(4):
            x = 4 * chip + k
            for h in range(2):
                for ref in (even, odd):
                    ref[x + 1, h, 0:8, :] = empty
                    ref[x + 1, h, 48:56, :] = empty
            for n, ref in enumerate((ym2_ref, ym1_ref, mid_ref, yp1_ref, yp2_ref)):
                rows = slice(8 * n, 8 * n + 8)
                padded = slice(8 * n + 8, 8 * n + 16)
                even[x + 1, 0, padded, :] = ref[chip, k]
                tail = pltpu.roll(ref[chip, 8], 112 - 32 * k, 1)
                even[x + 1, 1, padded, :] = jnp.where(tail_used, tail, 0.0)
                coef[x, 0, rows, :] = (ref[chip, 4 + k] - 1.0) * mask[0, rows, :]
                tail = pltpu.roll(ref[chip, 9], 112 - 32 * k, 1)
                coef[x, 1, rows, :] = (tail - 1.0) * mask[1, rows, :]
        return carry

    for chip in range(GX):
        fill(chip, 0)

    def put(m, chip, k, first, second):
        block = jnp.concatenate([first * mid_ref[chip, 10 + k], second * mid_ref[chip, 11 + k]], axis=0)
        high, middle, low = split_3(block)
        rows = slice(256 * (m % 4) + 32 * chip + 8 * k, 256 * (m % 4) + 32 * chip + 8 * k + 16)
        lhs[rows, 0:128] = middle
        lhs[rows, 128:256] = high
        lhs[rows, 256:384] = low

    def project(begin, end):
        size = 256 * (end - begin)
        rows = lhs[0:size, :]
        stacked = jnp.concatenate([rows[:, 0:256], rows[:, 0:256], rows[:, 128:384]], axis=1)
        total = jnp.dot(stacked, table_ref[...], preferred_element_type=f32)
        for m in range(begin, end):
            own = total[256 * (m - begin):256 * (m - begin + 1)]
            part_ref[m // 3, m % 3:m % 3 + 1, :] = jnp.sum(own * w_ref[...], axis=0, keepdims=True)

    def keep(m, ref):
        def one(p, carry):
            plane = jnp.clip(4 * gx - 7 + p, 0, NX + 1)
            held[m, p] = ref[plane, :, 16:40, :]
            return carry
        for p in range(20):
            one(p, 0)
        moves.append(pltpu.make_async_copy(held.at[m], kept_ref.at[m], sems.at[m]))
        moves[-1].start()

    def keep_coef(p, carry):
        x = 4 * gx - 8 + p
        real = ((x >= 0) & (x < NX)).astype(f32)
        held_a[p] = coef[jnp.clip(x, 0, NX - 1), :, 8:32, :] * real
        held_b[p] = mask[:, 8:32, :] * real
        return carry

    for p in range(20):
        keep_coef(p, 0)
    moves = [
        pltpu.make_async_copy(held_a, ka_ref, sems.at[BASIS + 1]),
        pltpu.make_async_copy(held_b, kb_ref, sems.at[BASIS + 2]),
    ]
    for move in moves:
        move.start()

    for x in range(0, NX, 2):
        put(0, x // 4, x % 4, even[x + 1, 0, 24:32, :], even[x + 2, 0, 24:32, :])
    keep(0, even)
    now, other = even, odd
    for m in range(1, DEGREE + 1):
        rows = (8, 48) if m <= BASIS else (16, 40)
        cut = slice(rows[0] - 8, rows[1] - 8)
        own = slice(24 - rows[0], 32 - rows[0])
        scale = lambda h: mask[h, cut, :]
        for x in range(0, NX, 2):
            pair = []
            for d in range(2):
                beside = beside_z(halves_of(now, x + d, rows))
                pair.append(next_plane(now, other, coef, scale, x + d, rows, m == 1, beside)[0][own])
            put(m, x // 4, x % 4, *pair)
        if m % 4 == 3:
            project(m - 3, m + 1)
        if m <= BASIS:
            keep(m, other)
        now, other = other, now
    project(DEGREE, DEGREE + 1)
    for move in moves:
        move.wait()


def total_of(value):
    return jnp.sum(jnp.sum(value, axis=0, keepdims=True), axis=1, keepdims=True)


def dot_of(left, right):
    product = left * right
    half = product.shape[1] // 2
    return total_of(product[:, :half] + product[:, half:])


def images_of(vectors):
    out = [7.0 * (vectors[0] + vectors[1])]
    for k in range(1, BASIS):
        out.append(7.0 * vectors[k] + 3.5 * (vectors[k + 1] + vectors[k - 1]))
    return out


def solve(columns, target):
    columns = list(columns)
    basis, upper, overlap, inverse = [], {}, {}, []
    for j in range(BASIS):
        column = columns[j]
        square = dot_of(column, column)
        if j:
            seen = [dot_of(basis[i], column) for i in range(j)]
            amounts = []
            for i in range(j):
                amount = seen[i]
                for k in range(i):
                    amount = amount - amounts[k] * overlap[i, k]
                amounts.append(amount)
            for i in range(j):
                column = column - amounts[i] * basis[i]
                upper[i, j] = upper[i, j] + amounts[i]
                spread = overlap[i, i] * amounts[i] - 2.0 * seen[i]
                for k in range(i):
                    spread = spread + (2.0 * overlap[i, k]) * amounts[k]
                square = square + spread * amounts[i]
        length = jnp.sqrt(jnp.maximum(square, 0.0) + tiny_value)
        inverse.append(1.0 / length)
        basis.append(column * inverse[j])
        for later in range(j + 1, BASIS):
            amount = dot_of(basis[j], columns[later])
            columns[later] = columns[later] - amount * basis[j]
            upper[j, later] = amount
        for k in range(j + 1):
            overlap[j, k] = dot_of(basis[j], basis[k])
    solved = [dot_of(vector, target) for vector in basis]
    for i in range(BASIS - 1, -1, -1):
        solved[i] = solved[i] * inverse[i]
        for k in range(i):
            solved[k] = solved[k] - upper[k, i] * solved[i]
    return solved


def remainder_of(solved):
    out = [-7.0 * c for c in solved] + [jnp.zeros_like(solved[0])]
    out[0] = out[0] + 1.0
    out[1] = out[1] - 7.0 * solved[0]
    for k in range(1, BASIS):
        out[k + 1] = out[k + 1] - 3.5 * solved[k]
        out[k - 1] = out[k - 1] - 3.5 * solved[k]
    return out


def finish_kernel(rows_ref, far_ref, far_a, far_b, sol_ref, res_ref, even, odd, kept_ref, ka_ref, kb_ref, sems):
    moves = [
        pltpu.make_async_copy(far, near, sems.at[n])
        for n, (far, near) in enumerate(((far_ref, kept_ref), (far_a, ka_ref), (far_b, kb_ref)))
    ]
    for move in moves:
        move.start()
    rows = []
    for m in range(DEGREE + 1):
        rows.append(jnp.concatenate(
            [rows_ref[GZ * chip + m // 3, m % 3:m % 3 + 1, :] for chip in range(GX)], axis=0
        ))
    for ref in (even, odd):
        for p in range(1, 21):
            for h in range(2):
                ref[p, h, 0:8, :] = jnp.zeros((8, 128), f32)
                ref[p, h, 32:40, :] = jnp.zeros((8, 128), f32)
    first = solve(images_of(rows[:BASIS + 1]), rows[0])
    rest = remainder_of(first)
    for move in moves:
        move.wait()
    for p in range(20):
        for h in range(2):
            value = rest[0] * kept_ref[0, p, h]
            for m in range(1, BASIS + 1):
                value = value + rest[m] * kept_ref[m, p, h]
            even[p + 1, h, 8:32, :] = value
    turned = []
    for j in range(BASIS + 1):
        value = rest[0] * rows[j]
        for m in range(1, BASIS + 1):
            value = value + (0.5 * rest[m]) * (rows[m + j] + rows[abs(m - j)])
        turned.append(value)
    fields = [[even[9 + p, 0, 16:24, :] for p in range(4)]]
    now, other = even, odd
    for m in range(1, BASIS + 1):
        fields.append([])
        for p in range(m, 20 - m):
            sides = beside_z(halves_of(now, p, (8, 32)))
            value = next_plane(now, other, ka_ref, lambda h: kb_ref[p, h], p, (8, 32), m == 1, sides)
            if 8 <= p < 12:
                fields[m].append(value[0][8:16])
        now, other = other, now
    second = solve(images_of(turned), turned[0])
    last = remainder_of(second)
    for p in range(4):
        value = first[0] * kept_ref[0, 8 + p, 0, 8:16, :]
        for m in range(1, BASIS):
            value = value + first[m] * kept_ref[m, 8 + p, 0, 8:16, :]
        for m in range(BASIS):
            value = value + second[m] * fields[m][p]
        sol_ref[p] = value
        value = last[0] * fields[0][p]
        for m in range(1, BASIS + 1):
            value = value + last[m] * fields[m][p]
        res_ref[p] = value


def run_basis(at, mid, sides, table, weights, interpret=False):
    return pl.pallas_call(
        basis_kernel,
        out_shape=[
            jax.ShapeDtypeStruct((GZ, 3, SHARE), f32),
            pltpu.HBM((BASIS + 1, 20, 2, 24, 128), f32),
            pltpu.HBM((20, 2, 24, 128), f32),
            pltpu.HBM((20, 2, 24, 128), f32),
        ],
        in_specs=[pl.BlockSpec(memory_space=pltpu.SMEM)] + [pl.BlockSpec(memory_space=VMEM)] * 7,
        out_specs=[pl.BlockSpec(memory_space=m) for m in (VMEM, pltpu.HBM, pltpu.HBM, pltpu.HBM)],
        scratch_shapes=[
            VMEM((NX + 2, 2, 56, 128), f32),
            VMEM((NX + 2, 2, 56, 128), f32),
            VMEM((NX, 2, 40, 128), f32),
            VMEM((2, 40, 128), f32),
            VMEM((1024, 384), bf16),
            VMEM((BASIS + 1, 20, 2, 24, 128), f32),
            VMEM((20, 2, 24, 128), f32),
            VMEM((20, 2, 24, 128), f32),
            pltpu.SemaphoreType.DMA((BASIS + 3,)),
        ],
        compiler_params=pltpu.CompilerParams(vmem_limit_bytes=28 << 20),
        name="basis",
        interpret=interpret,
    )(at, mid, *sides, table, weights)


def run_finish(rows, kept, ka, kb, interpret=False):
    return pl.pallas_call(
        finish_kernel,
        out_shape=[jax.ShapeDtypeStruct((4, 8, 128), f32)] * 2,
        in_specs=[pl.BlockSpec(memory_space=m) for m in (VMEM, pltpu.HBM, pltpu.HBM, pltpu.HBM)],
        out_specs=[pl.BlockSpec(memory_space=VMEM)] * 2,
        scratch_shapes=[
            VMEM((22, 2, 40, 128), f32),
            VMEM((22, 2, 40, 128), f32),
            VMEM((BASIS + 1, 20, 2, 24, 128), f32),
            VMEM((20, 2, 24, 128), f32),
            VMEM((20, 2, 24, 128), f32),
            pltpu.SemaphoreType.DMA((3,)),
        ],
        compiler_params=pltpu.CompilerParams(vmem_limit_bytes=60 << 20),
        name="finish",
        interpret=interpret,
    )(rows, kept, ka, kb)


def prepared_tables(freq_x, freq_y, freq_z, gx, gy, gz):
    mine = [lax.dynamic_slice_in_dim(f, gx * SHARE, SHARE) for f in (freq_x, freq_y, freq_z)]
    table_x = cosine_table(mine[0], 0, NX, NX)
    table_y = cosine_table(mine[1], gy * 8, 8, NY)
    table_z = cosine_table(mine[2], gz * 128, 128, NZ)
    high, middle, low = split_3(table_z)
    table = jnp.concatenate([high, high, middle, middle, low, high], axis=0)
    weights = (table_x[:, None, :] * table_y[None, :, :]).reshape(NX * 8, SHARE)
    return table, weights


def to_all(value, axis, size):
    return lax.all_to_all(
        jnp.broadcast_to(value[None], (size, *value.shape)), axis, 0, 0, tiled=True
    )


def tail_of(before, after):
    pieces = []
    for k in range(4):
        pieces += [before[:, k], after[:, k]]
    return jnp.concatenate(pieces, axis=-1)


def shards(right_side, diagonal, sign_bits, freq_x, freq_y, freq_z):
    gx, gy, gz = lax.axis_index("gx"), lax.axis_index(GY), lax.axis_index("gz")
    both = jnp.stack([right_side, diagonal])
    before = shifted(both[..., -16:], "gz", GZ, 1)
    after = shifted(both[..., :16], "gz", GZ, -1)
    signs = 1.0 - 2.0 * sign_bits.astype(f32)
    sent = jnp.concatenate([both.reshape(8, 8, 128), tail_of(before, after), signs], axis=0)
    mid = to_all(sent, "gx", GX)
    shared = mid[:, :10]
    sides = [shifted(shared, GY, 16, by) for by in (2, 1, -1, -2)]
    freq_x, freq_y, freq_z, mid = lax.optimization_barrier((freq_x, freq_y, freq_z, mid))
    table, weights = prepared_tables(freq_x, freq_y, freq_z, gx, gy, gz)
    at = jnp.stack([gx, gy, gz]).astype(jnp.int32)
    part, kept, ka, kb = run_basis(at, mid, sides, table, weights)
    rows = reduced(part)
    return tuple(run_finish(rows, kept, ka, kb))


def reduced(part):
    pieces = lax.all_to_all(part, "gz", 0, 0, tiled=True).sum(axis=0)
    pieces = to_all(pieces, GY, 16).sum(axis=0)
    return to_all(pieces, ("gx", "gz"), GX * GZ)


def solution(mesh):
    split = Mesh(
        mesh.devices.reshape(mesh.shape["gx"], 8, 2, mesh.shape["gz"]), ("gx", "gy_0", "gy_1", "gz")
    )
    return jax.shard_map(
        shards,
        mesh=split,
        in_specs=(P("gx", GY, "gz"), P("gx", GY, "gz"), P("gx", GY, "gz"), P(), P(), P()),
        out_specs=(P("gx", GY, "gz"), P("gx", GY, "gz")),
        check_vma=False,
    )
```
